32 devices in a mesh: grid: 8 (over y, x, core), rows: 4 (over z).
Axes of the slice: x: 2, y: 2, z: 4, core: 2. Of those that a mesh axis runs over, the one named last changes fastest.
Arguments:
- density: bfloat16 [32, 128, 4096], P(None, 'rows', 'grid'), as said below
- basis_values: bfloat16 [16, 16, 128, 512], P('grid', None, 'rows'), may hold values from -0.59765625 to 0.59765625
- grid_points: float32 [16, 3, 512], P('grid'), may hold values from -4 to 4
- grid_weights: float32 [16, 512], P('grid'), may hold values from 0.05 to 1
- screened_blocks: int32 [16, 16], P('grid'), may hold values from 0 to 31, as said below
Outputs:
- exchange: float32 [32, 128, 4096], P(None, 'rows', 'grid')
The draws below stay inside these ranges and needn't reach their ends.
Inputs may be any that keep to these rules, and one draw needn't show every extreme that they name: density is symmetric: density[a, i, b * 128 + j] equals density[b, j, a * 128 + i]. `screened_blocks`: each row holds 16 distinct block numbers.
All inputs are finite; a program needn't handle non-finite values.
Results may differ from the reference program's by a relative error of at most 0.00055.
The reference program's roundings to bfloat16 on the way count: a program that leaves them out, or rounds other values in their place, can miss the bound.
Values may be sent and summed in bfloat16 or wider, within the bound.
No kernel may reach another device: no remote copies, remote signals or barrier semaphores. Data moves between devices by JAX's collectives and lax.ppermute only.
A program may use at most 128 MiB of HBM per device.

```python
import math
import jax
import jax.numpy as jnp
from jax import lax

NBF = 4096
BS = 128
SIG = 16
PTS = 512
NBLK = 32
NBATCH = 16


def draw_density(key, part):
    key_off, key_diag = jax.random.split(jax.random.fold_in(key, 11), 2)
    noise = jax.random.normal(key_off, (NBF, NBF), jnp.float32) * (0.6 * (2.0 * NBF) ** (-0.5))
    dens = noise + noise.T
    diagonal = jax.random.uniform(key_diag, (NBF,), jnp.float32, 1.6, 2.6)
    dens = dens + jnp.diag(diagonal)
    return dens.reshape(NBF // BS, BS, NBF).astype(jnp.bfloat16)


def draw_screened_blocks(key, part):
    keys = jax.random.split(jax.random.fold_in(key, 7), NBATCH)
    picks = jax.vmap(lambda one_key: jax.random.permutation(one_key, NBF // BS)[:SIG])(keys)
    return picks.astype(jnp.int32)


def level_of(own_key, shape, cuts, least, largest):
    level = 1.0
    for position, shards_of in cuts:
        draws = jax.random.uniform(jax.random.fold_in(jax.random.fold_in(own_key, 6), position), (shards_of,), jnp.float32, least / len(cuts), largest / len(cuts))
        level = level * jnp.repeat(jnp.exp(draws), shape[position] // shards_of).reshape((-1,) + (1,) * (len(shape) - 1 - position))
    return level


def scatter_about(stream_key, extent, deviation, limit, cuts=(), dtype=jnp.bfloat16):
    values = deviation * jax.random.normal(stream_key, extent, jnp.float32)
    if cuts:
        values = values * level_of(stream_key, extent, cuts, -0.22, 0.18)
    return jnp.clip(values, -limit, limit).astype(dtype)


def setup_inputs(seed: int = 0) -> dict:
    key_of = jax.random.split(jax.random.key(seed), 6)
    return {
        "density": draw_density(jax.random.fold_in(key_of[5], 71), 0),
        "basis_values": scatter_about(key_of[1], (NBATCH, SIG, BS, PTS), 0.1, 0.59765625, ((0, 8), (2, 4))),
        "grid_points": jnp.clip(jax.random.uniform(key_of[2], (NBATCH, 3, PTS), jnp.float32, -4.0, 4.0) * level_of(key_of[2], (NBATCH, 3, PTS), ((0, 8),), -0.4, 0.0), -4.0, 4.0),
        "grid_weights": jnp.clip(jnp.exp(math.log(1.0) - 2.9957323 * jax.random.uniform(key_of[3], (NBATCH, PTS), jnp.float32) ** level_of(key_of[3], (NBATCH, PTS), ((0, 8),), -0.2, 0.2)), 0.05, 1.0),
        "screened_blocks": draw_screened_blocks(jax.random.fold_in(key_of[5], 71), 0),
    }


def reference(density, basis_values, grid_points, grid_weights, screened_blocks):
    dense = density.reshape(NBLK, BS, NBLK, BS)

    def one_batch(totals, items):
        values, places, weights, blocks = items
        chosen = dense[blocks][:, :, blocks, :].reshape(SIG * BS, SIG * BS)
        flat = values.reshape(SIG * BS, PTS)
        fmat = jnp.dot(chosen, flat, preferred_element_type=jnp.float32).astype(jnp.bfloat16)
        intersection = jnp.dot(flat.T, fmat, preferred_element_type=jnp.float32)
        diffs = places[:, :, None] - places[:, None, :]
        kern = 1.0 / jnp.sqrt(lax.optimization_barrier(jnp.sum(diffs * diffs, axis=0)) + 0.5)
        mixed = (weights[:, None] * kern * intersection).astype(jnp.bfloat16)
        potential = (jnp.dot(flat, mixed, preferred_element_type=jnp.float32) * weights[None, :]).astype(jnp.bfloat16)
        block_k = jnp.dot(flat, potential.T, preferred_element_type=jnp.float32).reshape(SIG, BS, SIG, BS)
        totals = totals.at[blocks[:, None], :, blocks[None, :], :].add(block_k.transpose(0, 2, 1, 3))
        return (totals, None)
    start_totals = jnp.zeros((NBLK, BS, NBLK, BS), jnp.float32)
    totals, unused = lax.scan(one_batch, start_totals, (basis_values, grid_points, grid_weights, screened_blocks))
    return totals.reshape(NBLK, BS, NBLK * BS)
```

```python
import functools

import jax
import jax.numpy as jnp
from jax import lax
from jax.experimental import pallas as pl
from jax.experimental.pallas import tpu as pltpu
from jax.sharding import PartitionSpec as P


F32 = jnp.float32
BF16 = jnp.bfloat16
LIMIT = 60 * 1024 * 1024
NT = (((1,), (1,)), ((), ()))
TN = (((0,), (0,)), ((), ()))


def line_forward(own, axis, count):
    up = [(i, i + 1) for i in range(count - 1)]
    down = [(i + 1, i) for i in range(count - 1)]
    from_low, from_high = [], []
    a = b = own
    for _ in range(count - 1):
        a = lax.ppermute(a, axis, up)
        b = lax.ppermute(b, axis, down)
        from_low.append(a)
        from_high.append(b)
    return from_low, from_high


def shift(value, axis, count, k):
    return lax.ppermute(value, axis, [(i, (i + k) % count) for i in range(count)])


def fmat_kernel(count, sel, place, stripe, own, *rest):
    low = rest[: count - 1]
    high = rest[count - 1 : 2 * (count - 1)]
    full, fmat, chosen = rest[2 * (count - 1) :]
    nb, nsig, rm, npts = own.shape
    cols = stripe.shape[3]
    bs = rm * count
    per = cols // bs
    z = place[0]
    full[:, :, z] = own[...]
    for k in range(1, count):

        @pl.when(z - k >= 0)
        def _():
            full[:, :, z - k] = low[k - 1][...]

        @pl.when(z + k < count)
        def _():
            full[:, :, z + k] = high[k - 1][...]

    for b in range(nb):
        for t in range(nsig):
            blk = sel[b, t]
            owner = blk // per
            start = pl.multiple_of((blk % per) * bs, bs)
            for s in range(nsig):
                chosen[pl.ds(s * rm, rm), pl.ds(t * bs, bs)] = stripe[owner, sel[b, s], :, pl.ds(start, bs)]
        x = full[b].reshape(nsig * bs, npts)
        fmat[b] = jnp.dot(chosen[...], x, preferred_element_type=F32).astype(BF16)


def mixed_kernel(count, place, full, cols3, rows3, weights, *rest):
    pieces, out = rest[:count], rest[count]
    nb, nsig, _, rm, npts = full.shape
    z = place[0]
    for b in range(nb):
        acc = None
        for k in range(count):
            src = lax.rem(z - k + count, count)
            x = full[b, :, src].reshape(nsig * rm, npts)
            part = lax.dot_general(pieces[k][b], x, TN, preferred_element_type=F32)
            acc = part if acc is None else acc + part
        total = None
        for c in range(3):
            d = rows3[b, c : c + 1, :] - cols3[b, :, c : c + 1]
            total = d * d if total is None else total + d * d
        kern = 1.0 / jnp.sqrt(total + 0.5)
        out[b] = (weights[b] * kern * acc).astype(BF16)


def exchange_kernel(count, sel, place, full, weights, *rest):
    pieces = rest[:count]
    keep, send, mixed, pot, bk = rest[count:]
    nb, nsig, _, rm, npts = full.shape
    bs = rm * count
    per = keep.shape[3] // bs
    z = place[0]
    g = place[1]
    keep[...] = jnp.zeros(keep.shape, F32)
    send[...] = jnp.zeros(send.shape, F32)
    for b in range(nb):
        for k in range(count):
            mixed[lax.rem(z - k + count, count)] = pieces[k][b]
        m = mixed[...].reshape(npts, npts)
        x = full[b].reshape(nsig * bs, npts)
        pot[...] = (lax.dot_general(x, m, NT, preferred_element_type=F32) * weights[b]).astype(BF16)
        mine = full[b, :, z].reshape(nsig * rm, npts)
        bk[...] = lax.dot_general(mine, pot[...], NT, preferred_element_type=F32)
        for t in range(nsig):
            blk = sel[b, t]
            rel = jnp.bitwise_xor(blk // per, g)
            slot = rel // 2
            start = pl.multiple_of((blk % per) * bs, bs)

            def add(ref):
                for s in range(nsig):
                    ref[slot, sel[b, s], :, pl.ds(start, bs)] += bk[pl.ds(s * rm, rm), pl.ds(t * bs, bs)]

            @pl.when(lax.rem(rel, 2) == 0)
            def _():
                add(keep)

            @pl.when(lax.rem(rel, 2) == 1)
            def _():
                add(send)


def halve(cur, bits, size):
    order = list(bits)
    dims = sorted(bits, reverse=True)
    for bit in order:
        at = dims.index(bit)
        keep = lax.index_in_dim(cur, 0, at, keepdims=False)
        send = lax.index_in_dim(cur, 1, at, keepdims=False)
        got = lax.ppermute(send, "grid", [(i, i ^ (1 << bit)) for i in range(size)])
        cur = keep + got
        dims.pop(at)
    return cur


def body(density, basis_values, grid_points, grid_weights, screened_blocks):
    nz = lax.axis_size("rows")
    ng = lax.axis_size("grid")
    z = lax.axis_index("rows")
    g = lax.axis_index("grid")
    nblocks, rm, cols = density.shape
    nb, nsig, _, npts = basis_values.shape
    bs = rm * nz
    share = npts // nz
    smem = pl.BlockSpec(memory_space=pltpu.SMEM)
    vmem = pl.BlockSpec(memory_space=pltpu.VMEM)
    params = pltpu.CompilerParams(vmem_limit_bytes=LIMIT)
    place = jnp.stack([z, g]).astype(jnp.int32)

    stripe = lax.all_gather(density, "grid", axis=0, tiled=False)
    low, high = line_forward(basis_values, "rows", nz)

    full, fmat = pl.pallas_call(
        functools.partial(fmat_kernel, nz),
        in_specs=[smem, smem] + [vmem] * (2 + 2 * (nz - 1)),
        out_specs=[vmem, vmem],
        out_shape=[
            jax.ShapeDtypeStruct((nb, nsig, nz, rm, npts), BF16),
            jax.ShapeDtypeStruct((nb, nsig * rm, npts), BF16),
        ],
        scratch_shapes=[pltpu.VMEM((nsig * rm, nsig * bs), BF16)],
        compiler_params=params,
        name="fmat",
    )(screened_blocks, place, stripe, basis_values, *low, *high)

    def part(k):
        return lax.dynamic_slice_in_dim(fmat, ((z + k) % nz) * share, share, axis=2)

    pieces = [part(0)] + [shift(part(k), "rows", nz, k) for k in range(1, nz)]
    own_points = lax.dynamic_slice_in_dim(grid_points, z * share, share, axis=2).transpose(0, 2, 1)
    weights = grid_weights[:, None, :]
    mixed = pl.pallas_call(
        functools.partial(mixed_kernel, nz),
        in_specs=[smem] + [vmem] * (4 + nz),
        out_specs=vmem,
        out_shape=jax.ShapeDtypeStruct((nb, share, npts), BF16),
        compiler_params=params,
        name="mixed",
    )(place, full, own_points, grid_points, weights, *pieces)

    shares = [mixed] + [shift(mixed, "rows", nz, k) for k in range(1, nz)]
    half = jax.ShapeDtypeStruct((ng // 2, nblocks, rm, cols), F32)
    keep, send = pl.pallas_call(
        functools.partial(exchange_kernel, nz),
        in_specs=[smem, smem] + [vmem] * (2 + nz),
        out_specs=[vmem, vmem],
        out_shape=[half, half],
        scratch_shapes=[
            pltpu.VMEM((nz, share, npts), BF16),
            pltpu.VMEM((nsig * bs, npts), BF16),
            pltpu.VMEM((nsig * rm, nsig * bs), F32),
        ],
        compiler_params=params,
        name="exchange",
    )(screened_blocks, place, full, weights, *shares)

    cur = keep + lax.ppermute(send, "grid", [(i, i ^ 1) for i in range(ng)])
    nbits = ng.bit_length() - 1
    bits = list(range(1, nbits))
    cur = cur.reshape((2,) * len(bits) + (nblocks, rm, cols))
    cut = nblocks // 2
    first = lax.slice_in_dim(cur, 0, cut, axis=len(bits))
    second = lax.slice_in_dim(cur, cut, nblocks, axis=len(bits))
    return jnp.concatenate([halve(first, bits, ng), halve(second, bits[::-1], ng)], axis=0)


def solution(mesh):
    size = mesh.shape["grid"]
    if size < 2 or size & (size - 1):
        raise ValueError("grid size")
    placed = (
        P(None, "rows", "grid"),
        P("grid", None, "rows", None),
        P("grid", None, None),
        P("grid", None),
        P("grid", None),
    )
    return jax.shard_map(
        body, mesh=mesh, in_specs=placed, out_specs=P(None, "rows", "grid"), check_vma=False
    )
```

```python
import functools

import jax
import jax.numpy as jnp
from jax import lax
from jax.experimental import pallas as pl
from jax.experimental.pallas import tpu as pltpu
from jax.sharding import PartitionSpec as P


F32 = jnp.float32
BF16 = jnp.bfloat16
F16 = jnp.float16
LIMIT = 60 * 1024 * 1024
NT = (((1,), (1,)), ((), ()))
TN = (((0,), (0,)), ((), ()))


def line_forward(own, axis, count):
    up = [(i, i + 1) for i in range(count - 1)]
    down = [(i + 1, i) for i in range(count - 1)]
    from_low, from_high = [], []
    a = b = own
    for _ in range(count - 1):
        a = lax.ppermute(a, axis, up)
        b = lax.ppermute(b, axis, down)
        from_low.append(a)
        from_high.append(b)
    return from_low, from_high


def shift(value, axis, count, k):
    return lax.ppermute(value, axis, [(i, (i + k) % count) for i in range(count)])


def fmat_kernel(count, sel, place, stripe, own, *rest):
    nb, nsig, rm, npts = own.shape
    low = rest[: nb * (count - 1)]
    high = rest[nb * (count - 1) : 2 * nb * (count - 1)]
    full, fmat, chosen = rest[2 * nb * (count - 1) :]
    cols = stripe.shape[3]
    bs = rm * count
    per = cols // bs
    z = place[0]
    full[:, :, z] = own[...]
    for b in range(nb):
        for k in range(1, count):

            @pl.when(z - k >= 0)
            def _():
                full[b, :, z - k] = low[b * (count - 1) + k - 1][...]

            @pl.when(z + k < count)
            def _():
                full[b, :, z + k] = high[b * (count - 1) + k - 1][...]

    for b in range(nb):
        for t in range(nsig):
            blk = sel[b, t]
            owner = blk // per
            start = pl.multiple_of((blk % per) * bs, bs)
            for s in range(nsig):
                chosen[pl.ds(s * rm, rm), pl.ds(t * bs, bs)] = stripe[owner, sel[b, s], :, pl.ds(start, bs)]
        x = full[b].reshape(nsig * bs, npts)
        fmat[b] = jnp.dot(chosen[...], x, preferred_element_type=F32).astype(BF16)


def mixed_kernel(count, place, full, cols3, rows3, weights, *rest):
    pieces, out = rest[:count], rest[count]
    nb, nsig, _, rm, npts = full.shape
    z = place[0]
    for b in range(nb):
        acc = None
        for k in range(count):
            src = lax.rem(z - k + count, count)
            x = full[b, :, src].reshape(nsig * rm, npts)
            part = lax.dot_general(pieces[k][b], x, TN, preferred_element_type=F32)
            acc = part if acc is None else acc + part
        total = None
        for c in range(3):
            d = rows3[b, c : c + 1, :] - cols3[b, :, c : c + 1]
            total = d * d if total is None else total + d * d
        kern = 1.0 / jnp.sqrt(total + 0.5)
        out[b] = (weights[b] * kern * acc).astype(BF16)


def exchange_kernel(count, sel, place, scale, full, weights, *rest):
    pieces = rest[:count]
    keep, send, mixed, pot, bk = rest[count:]
    nb, nsig, _, rm, npts = full.shape
    bs = rm * count
    per = keep.shape[3] // bs
    z = place[0]
    g = place[1]
    keep[...] = jnp.zeros(keep.shape, F32)
    send[...] = jnp.zeros(send.shape, F32)
    for b in range(nb):
        for k in range(count):
            mixed[lax.rem(z - k + count, count)] = pieces[k][b]
        m = mixed[...].reshape(npts, npts)
        x = full[b].reshape(nsig * bs, npts)
        pot[...] = (lax.dot_general(x, m, NT, preferred_element_type=F32) * weights[b]).astype(BF16)
        mine = full[b, :, z].reshape(nsig * rm, npts)
        bk[...] = lax.dot_general(mine, pot[...], NT, preferred_element_type=F32) * scale[0]
        for t in range(nsig):
            blk = sel[b, t]
            rel = jnp.bitwise_xor(blk // per, g)
            slot = rel // 2
            start = pl.multiple_of((blk % per) * bs, bs)

            def add(ref):
                for s in range(nsig):
                    ref[slot, sel[b, s], :, pl.ds(start, bs)] += bk[pl.ds(s * rm, rm), pl.ds(t * bs, bs)]

            @pl.when(lax.rem(rel, 2) == 0)
            def _():
                add(keep)

            @pl.when(lax.rem(rel, 2) == 1)
            def _():
                add(send)


def halve(cur, bits, size):
    order = list(bits)
    dims = sorted(bits, reverse=True)
    for bit in order:
        at = dims.index(bit)
        keep = lax.index_in_dim(cur, 0, at, keepdims=False)
        send = lax.index_in_dim(cur, 1, at, keepdims=False)
        got = lax.ppermute(send.astype(F16), "grid", [(i, i ^ (1 << bit)) for i in range(size)])
        cur = keep + got.astype(F32)
        dims.pop(at)
    return cur


def body(density, basis_values, grid_points, grid_weights, screened_blocks):
    nz = lax.axis_size("rows")
    ng = lax.axis_size("grid")
    z = lax.axis_index("rows")
    g = lax.axis_index("grid")
    nblocks, rm, cols = density.shape
    nb, nsig, _, npts = basis_values.shape
    bs = rm * nz
    share = npts // nz
    smem = pl.BlockSpec(memory_space=pltpu.SMEM)
    vmem = pl.BlockSpec(memory_space=pltpu.VMEM)
    params = pltpu.CompilerParams(vmem_limit_bytes=LIMIT)
    place = jnp.stack([z, g]).astype(jnp.int32)

    stripe = lax.all_gather(density, "grid", axis=0, tiled=False)
    chains = [line_forward(basis_values[b], "rows", nz) for b in range(nb)]
    low = [c for chain in chains for c in chain[0]]
    high = [c for chain in chains for c in chain[1]]

    full, fmat = pl.pallas_call(
        functools.partial(fmat_kernel, nz),
        in_specs=[smem, smem] + [vmem] * (2 + 2 * nb * (nz - 1)),
        out_specs=[vmem, vmem],
        out_shape=[
            jax.ShapeDtypeStruct((nb, nsig, nz, rm, npts), BF16),
            jax.ShapeDtypeStruct((nb, nsig * rm, npts), BF16),
        ],
        scratch_shapes=[pltpu.VMEM((nsig * rm, nsig * bs), BF16)],
        compiler_params=params,
        name="fmat",
    )(screened_blocks, place, stripe, basis_values, *low, *high)

    def part(k):
        return lax.dynamic_slice_in_dim(fmat, ((z + k) % nz) * share, share, axis=2)

    pieces = [part(0)] + [shift(part(k), "rows", nz, k) for k in range(1, nz)]
    own_points = lax.dynamic_slice_in_dim(grid_points, z * share, share, axis=2).transpose(0, 2, 1)
    weights = grid_weights[:, None, :]
    mixed = pl.pallas_call(
        functools.partial(mixed_kernel, nz),
        in_specs=[smem] + [vmem] * (4 + nz),
        out_specs=vmem,
        out_shape=jax.ShapeDtypeStruct((nb, share, npts), BF16),
        compiler_params=params,
        name="mixed",
    )(place, full, own_points, grid_points, weights, *pieces)

    x32 = basis_values.astype(F32)
    norm = jnp.max(jnp.sum(x32 * x32, axis=3))
    peak = jnp.max(jnp.abs(mixed)).astype(F32)
    norm, peak = lax.pmax(jnp.stack([norm, peak]), ("grid", "rows"))
    bound = jnp.maximum(norm, 1e-30) * float(npts * nb * ng)
    scale = jnp.clip(2.0**14 / bound / jnp.maximum(peak, 1e-30), 2.0**-120, 2.0**110)

    shares = [mixed] + [shift(mixed, "rows", nz, k) for k in range(1, nz)]
    half = jax.ShapeDtypeStruct((ng // 2, nblocks, rm, cols), F32)
    keep, send = pl.pallas_call(
        functools.partial(exchange_kernel, nz),
        in_specs=[smem, smem, smem] + [vmem] * (2 + nz),
        out_specs=[vmem, vmem],
        out_shape=[half, half],
        scratch_shapes=[
            pltpu.VMEM((nz, share, npts), BF16),
            pltpu.VMEM((nsig * bs, npts), BF16),
            pltpu.VMEM((nsig * rm, nsig * bs), F32),
        ],
        compiler_params=params,
        name="exchange",
    )(screened_blocks, place, scale[None], full, weights, *shares)

    cur = keep + lax.ppermute(send, "grid", [(i, i ^ 1) for i in range(ng)])
    nbits = ng.bit_length() - 1
    bits = list(range(1, nbits))
    cur = cur.reshape((2,) * len(bits) + (nblocks, rm, cols))
    cut = nblocks // 2
    first = lax.slice_in_dim(cur, 0, cut, axis=len(bits))
    second = lax.slice_in_dim(cur, cut, nblocks, axis=len(bits))
    return jnp.concatenate([halve(first, bits, ng), halve(second, bits[::-1], ng)], axis=0) * (1.0 / scale)


def solution(mesh):
    size = mesh.shape["grid"]
    if size < 2 or size & (size - 1):
        raise ValueError("grid size")
    placed = (
        P(None, "rows", "grid"),
        P("grid", None, "rows", None),
        P("grid", None, None),
        P("grid", None),
        P("grid", None),
    )
    return jax.shard_map(
        body, mesh=mesh, in_specs=placed, out_specs=P(None, "rows", "grid"), check_vma=False
    )
```

```python
import functools

import jax
import jax.numpy as jnp
from jax import lax
from jax.experimental import pallas as pl
from jax.experimental.pallas import tpu as pltpu
from jax.sharding import PartitionSpec as P


F32 = jnp.float32
BF16 = jnp.bfloat16
F16 = jnp.float16
LIMIT = 60 * 1024 * 1024
NT = (((1,), (1,)), ((), ()))
TN = (((0,), (0,)), ((), ()))


def line_forward(own, axis, count):
    up = [(i, i + 1) for i in range(count - 1)]
    down = [(i + 1, i) for i in range(count - 1)]
    from_low, from_high = [], []
    a = b = own
    for _ in range(count - 1):
        a = lax.ppermute(a, axis, up)
        b = lax.ppermute(b, axis, down)
        from_low.append(a)
        from_high.append(b)
    return from_low, from_high


def shift(value, axis, count, k):
    return lax.ppermute(value, axis, [(i, (i + k) % count) for i in range(count)])


def fmat_kernel(count, sel, place, stripe, own, *rest):
    nb, nsig, rm, npts = own.shape
    low = rest[: nb * (count - 1)]
    high = rest[nb * (count - 1) : 2 * nb * (count - 1)]
    full, fmat, chosen = rest[2 * nb * (count - 1) :]
    cols = stripe.shape[3]
    bs = rm * count
    per = cols // bs
    z = place[0]
    full[:, :, z] = own[...]
    for b in range(nb):
        for k in range(1, count):

            @pl.when(z - k >= 0)
            def _():
                full[b, :, z - k] = low[b * (count - 1) + k - 1][...]

            @pl.when(z + k < count)
            def _():
                full[b, :, z + k] = high[b * (count - 1) + k - 1][...]

    for b in range(nb):
        for t in range(nsig):
            blk = sel[b, t]
            owner = blk // per
            start = pl.multiple_of((blk % per) * bs, bs)
            for s in range(nsig):
                chosen[pl.ds(s * rm, rm), pl.ds(t * bs, bs)] = stripe[owner, sel[b, s], :, pl.ds(start, bs)]
        x = full[b].reshape(nsig * bs, npts)
        fmat[b] = jnp.dot(chosen[...], x, preferred_element_type=F32).astype(BF16)


def mixed_kernel(count, place, full, cols3, rows3, weights, *rest):
    pieces, out = rest[:count], rest[count]
    nb, nsig, _, rm, npts = full.shape
    z = place[0]
    for b in range(nb):
        acc = None
        for k in range(count):
            src = lax.rem(z - k + count, count)
            x = full[b, :, src].reshape(nsig * rm, npts)
            part = lax.dot_general(pieces[k][b], x, TN, preferred_element_type=F32)
            acc = part if acc is None else acc + part
        total = None
        for c in range(3):
            d = rows3[b, c : c + 1, :] - cols3[b, :, c : c + 1]
            total = d * d if total is None else total + d * d
        kern = 1.0 / jnp.sqrt(total + 0.5)
        out[b] = (weights[b] * kern * acc).astype(BF16)


def exchange_kernel(count, sel, place, full, weights, *rest):
    pieces = rest[:count]
    keep, send, mixed, pot, bk = rest[count:]
    nb, nsig, _, rm, npts = full.shape
    bs = rm * count
    per = keep.shape[3] // bs
    z = place[0]
    g = place[1]
    keep[...] = jnp.zeros(keep.shape, F32)
    send[...] = jnp.zeros(send.shape, F32)
    for b in range(nb):
        for k in range(count):
            mixed[lax.rem(z - k + count, count)] = pieces[k][b]
        m = mixed[...].reshape(npts, npts)
        x = full[b].reshape(nsig * bs, npts)
        pot[...] = (lax.dot_general(x, m, NT, preferred_element_type=F32) * weights[b]).astype(BF16)
        mine = full[b, :, z].reshape(nsig * rm, npts)
        bk[...] = lax.dot_general(mine, pot[...], NT, preferred_element_type=F32)
        for t in range(nsig):
            blk = sel[b, t]
            rel = jnp.bitwise_xor(blk // per, g)
            slot = rel // 2
            start = pl.multiple_of((blk % per) * bs, bs)

            def add(ref):
                for s in range(nsig):
                    ref[slot, sel[b, s], :, pl.ds(start, bs)] += bk[pl.ds(s * rm, rm), pl.ds(t * bs, bs)]

            @pl.when(lax.rem(rel, 2) == 0)
            def _():
                add(keep)

            @pl.when(lax.rem(rel, 2) == 1)
            def _():
                add(send)


def scale_of(bound):
    norm, peak = bound[:, 0:1], bound[:, 1:2]
    scale = 2.0**14 / jnp.maximum(norm, 1e-30) / jnp.maximum(peak, 1e-30)
    return jnp.clip(scale, 2.0**-120, 2.0**110)


def merge(a, b):
    return jnp.concatenate([jnp.maximum(a[:, 0:1], b[:, 0:1]), a[:, 1:2] + b[:, 1:2]], axis=1)


def halve(cur, bits, size, bound):
    dims = sorted(bits, reverse=True)
    for bit in bits:
        pairs = [(i, i ^ (1 << bit)) for i in range(size)]
        at = dims.index(bit)
        keep = lax.index_in_dim(cur, 0, at, keepdims=False)
        send = lax.index_in_dim(cur, 1, at, keepdims=False)
        other = lax.ppermute(bound, "grid", pairs)
        got = lax.ppermute((send * scale_of(bound)[0, 0]).astype(F16), "grid", pairs)
        cur = keep + got.astype(F32) * (1.0 / scale_of(other)[0, 0])
        bound = merge(bound, other)
        dims.pop(at)
    return cur


def body(density, basis_values, grid_points, grid_weights, screened_blocks):
    nz = lax.axis_size("rows")
    ng = lax.axis_size("grid")
    z = lax.axis_index("rows")
    g = lax.axis_index("grid")
    nblocks, rm, cols = density.shape
    nb, nsig, _, npts = basis_values.shape
    bs = rm * nz
    share = npts // nz
    smem = pl.BlockSpec(memory_space=pltpu.SMEM)
    vmem = pl.BlockSpec(memory_space=pltpu.VMEM)
    params = pltpu.CompilerParams(vmem_limit_bytes=LIMIT)
    place = jnp.stack([z, g]).astype(jnp.int32)

    stripe = lax.all_gather(density, "grid", axis=0, tiled=False)
    chains = [line_forward(basis_values[b], "rows", nz) for b in range(nb)]
    low = [c for chain in chains for c in chain[0]]
    high = [c for chain in chains for c in chain[1]]

    full, fmat = pl.pallas_call(
        functools.partial(fmat_kernel, nz),
        in_specs=[smem, smem] + [vmem] * (2 + 2 * nb * (nz - 1)),
        out_specs=[vmem, vmem],
        out_shape=[
            jax.ShapeDtypeStruct((nb, nsig, nz, rm, npts), BF16),
            jax.ShapeDtypeStruct((nb, nsig * rm, npts), BF16),
        ],
        scratch_shapes=[pltpu.VMEM((nsig * rm, nsig * bs), BF16)],
        compiler_params=params,
        name="fmat",
    )(screened_blocks, place, stripe, basis_values, *low, *high)

    def part(k):
        return lax.dynamic_slice_in_dim(fmat, ((z + k) % nz) * share, share, axis=2)

    pieces = [part(0)] + [shift(part(k), "rows", nz, k) for k in range(1, nz)]
    own_points = lax.dynamic_slice_in_dim(grid_points, z * share, share, axis=2).transpose(0, 2, 1)
    weights = grid_weights[:, None, :]
    mixed = pl.pallas_call(
        functools.partial(mixed_kernel, nz),
        in_specs=[smem] + [vmem] * (4 + nz),
        out_specs=vmem,
        out_shape=jax.ShapeDtypeStruct((nb, share, npts), BF16),
        compiler_params=params,
        name="mixed",
    )(place, full, own_points, grid_points, weights, *pieces)

    shares = [mixed] + [shift(mixed, "rows", nz, k) for k in range(1, nz)]
    half = jax.ShapeDtypeStruct((ng // 2, nblocks, rm, cols), F32)
    keep, send = pl.pallas_call(
        functools.partial(exchange_kernel, nz),
        in_specs=[smem, smem] + [vmem] * (2 + nz),
        out_specs=[vmem, vmem],
        out_shape=[half, half],
        scratch_shapes=[
            pltpu.VMEM((nz, share, npts), BF16),
            pltpu.VMEM((nsig * bs, npts), BF16),
            pltpu.VMEM((nsig * rm, nsig * bs), F32),
        ],
        compiler_params=params,
        name="exchange",
    )(screened_blocks, place, full, weights, *shares)

    x32 = full.astype(F32)
    norm = jnp.max(jnp.sum(x32 * x32, axis=4)) * float(npts * nb)
    peak = functools.reduce(jnp.maximum, [jnp.max(jnp.abs(m)).astype(F32) for m in shares])
    bound = jnp.broadcast_to(jnp.stack([norm, peak])[None], (8, 2))
    swap = [(i, i ^ 1) for i in range(ng)]
    bound = merge(bound, lax.ppermute(bound, "grid", swap))
    cur = keep + lax.ppermute(send, "grid", swap)
    nbits = ng.bit_length() - 1
    bits = list(range(1, nbits))
    cur = cur.reshape((2,) * len(bits) + (nblocks, rm, cols))
    cut = nblocks // 2
    first = lax.slice_in_dim(cur, 0, cut, axis=len(bits))
    second = lax.slice_in_dim(cur, cut, nblocks, axis=len(bits))
    return jnp.concatenate([halve(first, bits, ng, bound), halve(second, bits[::-1], ng, bound)], axis=0)


def solution(mesh):
    size = mesh.shape["grid"]
    if size < 2 or size & (size - 1):
        raise ValueError("grid size")
    placed = (
        P(None, "rows", "grid"),
        P("grid", None, "rows", None),
        P("grid", None, None),
        P("grid", None),
        P("grid", None),
    )
    return jax.shard_map(
        body, mesh=mesh, in_specs=placed, out_specs=P(None, "rows", "grid"), check_vma=False
    )
```
